32 devices in a mesh: ctx: 8 (over z, y), tp: 4 (over x, core).
Axes of the slice: x: 2, y: 2, z: 4, core: 2. Of those that a mesh axis runs over, the one named last changes fastest.
Arguments:
- queries: bfloat16 [2048, 64, 128], P('ctx', 'tp'), may hold values from -48 to 48
- keys: bfloat16 [2048, 8, 128], P('ctx', 'tp'), may hold values from -3 to 3
- values: bfloat16 [2048, 8, 128], P('ctx', 'tp'), may hold values from -6 to 6
- segment_ids: int32 [2048], P('ctx'), may hold values from 0 to 7, never falling along the last dimension, each value on 1 to 1280 neighbouring positions
Outputs:
- attended: bfloat16 [2048, 8192], P(('ctx', 'tp'))
The draws below stay inside these ranges and needn't reach their ends.
Inputs may be any that keep to these rules, and one draw needn't show every extreme that they name: `segment_ids`: ids never fall along the tokens; each document holds 1 to 1280 tokens, and one holds exactly 1280.
All inputs are finite; a program needn't handle non-finite values.
Results may differ from the reference program's by a relative error of at most 0.003.
Values may be sent and summed in bfloat16 or wider, within the bound.
A program may use at most 64 MiB of HBM per device.

```python
import math
import jax
import jax.numpy as jnp
import numpy as np
from jax import lax

QUERY_HEADS = 64
KEY_VALUE_HEADS = 8
HEAD_SIZE = 128
DOCS = 8
PACK_TOKENS = 2048
MOST = 1280


def paired_draw(key):
    base = jax.random.fold_in(key, 4242)
    key_random_keys, key_query = jax.random.split(base, 2)
    keys = jnp.clip(jax.random.normal(key_random_keys, (PACK_TOKENS, KEY_VALUE_HEADS, HEAD_SIZE), jnp.float32), -3.0, 3.0)
    queries = jnp.clip(2.5 * jax.random.normal(key_query, (PACK_TOKENS, QUERY_HEADS, HEAD_SIZE), jnp.float32), -12.0, 12.0)
    return (queries.astype(jnp.bfloat16), keys.astype(jnp.bfloat16))


def draw_queries(key, part):
    return paired_draw(key)[0]


def draw_keys(key, part):
    return paired_draw(key)[1]


def shard_levels(own_key, extent, cuts, least, high):
    loudness, own = 1.0, jax.random.fold_in(own_key, 6)
    for position, shards_of in cuts:
        heights = jnp.exp(jax.random.uniform(jax.random.fold_in(own, position), (shards_of,), jnp.float32, least / len(cuts), high / len(cuts)))
        loudness = loudness * jnp.repeat(heights, extent[position] // shards_of).reshape([-1 if axis == position else 1 for axis in range(len(extent))])
    return loudness


def length_profile(count, total, most, lean):
    weights = [(1 << 20) // math.isqrt(standing ** lean) + 1 for standing in range(2, count + 1)]
    spare, given = total - most - (count - 1), [1] * (count - 1)
    while spare > 0:
        free = [i for i in range(count - 1) if given[i] < most]
        mass, remaining = sum([weights[i] for i in free]), spare
        for i in free:
            addition = min(most - given[i], max(1, remaining * weights[i] // mass), spare)
            given[i] = given[i] + addition
            spare = spare - addition
    return np.array([most] + given)


def uneven(rng, amount, total, limit, skew):
    if amount == 2:
        one = jax.random.randint(rng, (), max(1, total - limit), min(limit, total - 1) + 1)
        return jnp.stack([one, total - one])
    lengths = jnp.asarray(length_profile(amount, total, limit, skew), jnp.int32)
    couples = (amount - 1) // 2
    donor, taker = lengths[1:1 + 2 * couples:2], lengths[2:2 + 2 * couples:2]
    room = jnp.minimum(donor - 1, limit - taker)
    moved = jax.random.randint(jax.random.fold_in(rng, 1), (couples,), 0, 1 << 20) % (room + 1)
    lengths = lengths.at[1:1 + 2 * couples:2].set(donor - moved).at[2:2 + 2 * couples:2].set(taker + moved)
    return lengths[jax.random.permutation(jax.random.fold_in(rng, 2), amount)]


def scatter_about(key, extent, deviation, limit, shards=(), kind=jnp.bfloat16):
    gain = shard_levels(key, extent, shards, -0.22, 0.18) if shards else 1.0
    values = jax.random.normal(key, extent, jnp.float32) * deviation * gain
    return jnp.minimum(jnp.maximum(values, -limit), limit).astype(kind)


def setup_inputs(seed: int = 0) -> dict:
    arg_keys = jax.random.split(jax.random.key(seed), 5)
    return {
        "queries": draw_queries(jax.random.fold_in(arg_keys[4], 71), 0),
        "keys": draw_keys(jax.random.fold_in(arg_keys[4], 71), 0),
        "values": scatter_about(arg_keys[2], (PACK_TOKENS, KEY_VALUE_HEADS, HEAD_SIZE), 1.0, 6.0, ((0, 8), (1, 4))),
        "segment_ids": jnp.searchsorted(jnp.cumsum(uneven(arg_keys[3], DOCS, PACK_TOKENS, MOST, 2)), jnp.arange(PACK_TOKENS), side="right").astype(jnp.int32),
    }


def reference(queries, keys, values, segment_ids):
    tokens, heads, head = queries.shape
    groups = keys.shape[1]
    per_group = heads // groups
    block = math.gcd(tokens, 512)
    positions = jnp.arange(tokens, dtype=jnp.int32)
    scale = 1.0 / math.sqrt(head)

    def one_block(index):
        first = (index * block).astype(jnp.int32)
        query_rows = lax.dynamic_slice_in_dim(queries, first, block, 0).reshape(block, groups, per_group, head)
        seg_rows = lax.dynamic_slice_in_dim(segment_ids, first, block, 0)
        pos_rows = first + jnp.arange(block, dtype=jnp.int32)
        allowed = (seg_rows[:, None] == segment_ids[None, :]) & (positions[None, :] <= pos_rows[:, None])

        def one_group(group):
            query_group = lax.dynamic_index_in_dim(query_rows, group, 1, keepdims=False).astype(jnp.float32)
            key_group = lax.dynamic_index_in_dim(keys, group, 1, keepdims=False).astype(jnp.float32)
            value_group = lax.dynamic_index_in_dim(values, group, 1, keepdims=False).astype(jnp.float32)
            scores = jnp.einsum('tgd,pd->gtp', query_group, key_group) * scale
            scores = jnp.where(allowed[None], scores, -1e+30)
            top = lax.optimization_barrier(jnp.max(scores, axis=-1))
            weights = jnp.where(allowed[None], jnp.exp(scores - top[..., None]), 0.0)
            total = lax.optimization_barrier(jnp.sum(weights, axis=-1))
            rounded = lax.optimization_barrier(weights.astype(jnp.bfloat16)).astype(jnp.float32)
            mixed = jnp.einsum('gtp,pd->gtd', rounded, value_group)
            return mixed / total[..., None]
        result = lax.map(one_group, jnp.arange(groups, dtype=jnp.int32))
        return jnp.transpose(result, (2, 0, 1, 3)).reshape(block, heads * head).astype(jnp.bfloat16)
    output = lax.map(one_block, jnp.arange(tokens // block, dtype=jnp.int32))
    return output.reshape(tokens, heads * head)
```

```python
import functools
import math

import jax
import jax.numpy as jnp
from jax import lax
from jax.experimental import pallas as pl
from jax.experimental.pallas import tpu as pltpu
from jax.sharding import PartitionSpec as P

MESH = pl.DeviceIdType.MESH
NEG = -1e30


def plane_width(mesh):
    n = mesh.shape["ctx"]
    try:
        width = len({d.coords[1] for d in mesh.devices.flat})
    except Exception:
        width = 2
    return width if n % width == 0 else 1


def kernel(cfg, q_ref, kv_ref, seg_ref, segcol_ref, out_ref,
           buf, segs, bias, acc, top, o_buf,
           kv_send, kv_recv, seg_send, seg_recv, o_send, o_recv, o_local):
    n, ny, reach, tp, groups, per_group, rows, head = cfg
    nz = n // ny
    depth = min(nz - 1, (reach + ny - 1) // ny) + 1
    out_rows = rows // tp
    const = math.log2(math.e) / math.sqrt(head)
    me = lax.axis_index("ctx")
    mt = lax.axis_index("tp")
    z = me // ny
    y = me % ny

    barrier = pltpu.get_barrier_semaphore()
    for d in range(1, reach + 1):
        @pl.when(me + d < n)
        def _():
            pl.semaphore_signal(barrier, inc=1, device_id={"ctx": me + d, "tp": mt}, device_id_type=MESH)

        @pl.when(me - d >= 0)
        def _():
            pl.semaphore_signal(barrier, inc=1, device_id={"ctx": me - d, "tp": mt}, device_id_type=MESH)
    for e in range(1, tp):
        pl.semaphore_signal(barrier, inc=1, device_id={"ctx": me, "tp": (mt + e) % tp}, device_id_type=MESH)
    peers = (tp - 1) + jnp.minimum(n - 1 - me, reach) + jnp.minimum(me, reach)
    pl.semaphore_wait(barrier, peers)

    def piece(s, dy, g, w):
        if s == 0 and dy == 0:
            return kv_ref.at[g, w]
        return buf.at[s * ny + dy, g, w]

    def sem_index(s, dy, g, w):
        return ((s * ny + dy) * groups + g) * 2 + w

    def send_index(s, e, g, w):
        return ((s * ny + e) * groups + g) * 2 + w

    def z_copy(s, g, w):
        return pltpu.make_async_remote_copy(
            src_ref=piece(s, 0, g, w),
            dst_ref=buf.at[(s + 1) * ny, g, w],
            send_sem=kv_send.at[send_index(s, 0, g, w)],
            recv_sem=kv_recv.at[sem_index(s + 1, 0, g, w)],
            device_id={"ctx": me + ny, "tp": mt},
            device_id_type=MESH,
        )

    def y_copy(s, e, g, w):
        return pltpu.make_async_remote_copy(
            src_ref=piece(s, 0, g, w),
            dst_ref=buf.at[s * ny + ny - e, g, w],
            send_sem=kv_send.at[send_index(s, e, g, w)],
            recv_sem=kv_recv.at[sem_index(s, ny - e, g, w)],
            device_id={"ctx": z * ny + (y + e) % ny, "tp": mt},
            device_id_type=MESH,
        )

    def owner(s, dy):
        return (z - s) * ny + (y + dy) % ny

    def has_column(s):
        return (z >= s) & (z * ny - owner(s, 0) <= reach)

    def sends_z(s):
        return (z >= s) & (z + 1 < nz) & ((z + 1) * ny - owner(s, 0) <= reach)

    def sends_y(s, e):
        gap = z * ny + (y + e) % ny - owner(s, 0)
        return (z >= s) & (gap > 0) & (gap <= reach)

    def wanted(s, dy):
        gap = me - owner(s, dy)
        return (z >= s) & (gap > 0) & (gap <= reach)

    def arrived(s, dy, g, w):
        pltpu.make_async_copy(buf.at[s * ny + dy, g, w], buf.at[s * ny + dy, g, w],
                              kv_recv.at[sem_index(s, dy, g, w)]).wait()

    def push(s, g):
        for w in range(2):
            if s > 0:
                @pl.when(has_column(s))
                def _():
                    arrived(s, 0, g, w)
            if s + 1 < depth:
                @pl.when(sends_z(s))
                def _():
                    z_copy(s, g, w).start()
            for e in range(1, ny):
                @pl.when(sends_y(s, e))
                def _():
                    y_copy(s, e, g, w).start()

    def seg_copy(d):
        return pltpu.make_async_remote_copy(
            src_ref=seg_ref,
            dst_ref=segs.at[d],
            send_sem=seg_send.at[d],
            recv_sem=seg_recv.at[d],
            device_id={"ctx": me + d, "tp": mt},
            device_id_type=MESH,
        )

    push(0, 0)
    for d in range(1, reach + 1):
        @pl.when(me + d < n)
        def _():
            seg_copy(d).start()

    def attend(s, dy, g, first):
        k_ref, v_ref = piece(s, dy, g, 0), piece(s, dy, g, 1)
        if first:
            seg_k = seg_ref[...]
        else:
            seg_k = segs[me - owner(s, dy)]
        allowed = segcol_ref[...] == seg_k
        if first:
            r = lax.broadcasted_iota(jnp.int32, (rows, rows), 0)
            c = lax.broadcasted_iota(jnp.int32, (rows, rows), 1)
            allowed = allowed & (c <= r)
        bias[...] = jnp.where(allowed, 0.0, NEG)

        def one(h, carry):
            i = g * per_group + h
            scores = lax.dot_general(q_ref[i], k_ref[...], (((1,), (1,)), ((), ())),
                                     preferred_element_type=jnp.float32)
            scores = scores * const + bias[...]
            high = jnp.max(scores, axis=1, keepdims=True)
            if not first:
                old = top[i][:, :1]
                high = jnp.maximum(old, high)
            weights = jnp.exp2(scores - high).astype(jnp.bfloat16)
            v = jnp.concatenate([v_ref[...], jnp.ones((rows, head), jnp.bfloat16)], axis=1)
            mixed = jnp.dot(weights, v, preferred_element_type=jnp.float32)
            if not first:
                mixed = acc[i] * jnp.exp2(old - high) + mixed
            acc[i] = mixed
            top[i] = jnp.broadcast_to(high, (rows, head))
            return carry

        lax.fori_loop(0, per_group, one, 0, unroll=2)

    def attend_y(s, g):
        for dy in range(1, ny):
            @pl.when(wanted(s, dy))
            def _():
                arrived(s, dy, g, 0)
                arrived(s, dy, g, 1)
                attend(s, dy, g, False)

    per_send = max(per_group // 2, 1)
    width = per_send * head
    pieces = per_group // per_send

    def o_copy(c, e):
        col = pl.multiple_of((mt * groups * pieces + c) * width, width)
        to = (mt + e) % tp
        return pltpu.make_async_remote_copy(
            src_ref=o_buf.at[pl.ds(pl.multiple_of(to * out_rows, out_rows), out_rows), pl.ds(c * width, width)],
            dst_ref=out_ref.at[:, pl.ds(col, width)],
            send_sem=o_send.at[c * tp + e],
            recv_sem=o_recv.at[c * tp + e],
            device_id={"ctx": me, "tp": to},
            device_id_type=MESH,
        )

    def o_own(c):
        col = pl.multiple_of((mt * groups * pieces + c) * width, width)
        return pltpu.make_async_copy(
            o_buf.at[pl.ds(pl.multiple_of(mt * out_rows, out_rows), out_rows), pl.ds(c * width, width)],
            out_ref.at[:, pl.ds(col, width)],
            o_local.at[c],
        )

    def finish(g):
        for p in range(pieces):
            c = g * pieces + p
            for h in range(per_send):
                i = g * per_group + p * per_send + h
                o_buf[:, i * head:(i + 1) * head] = (acc[i, :, :head] / acc[i, :, head:]).astype(jnp.bfloat16)
            for e in range(1, tp):
                o_copy(c, e).start()
            o_own(c).start()

    for g in range(groups):
        attend(0, 0, g, True)
        if g == 0:
            for d in range(1, reach + 1):
                @pl.when(me - d >= 0)
                def _():
                    pltpu.make_async_copy(segs.at[d], segs.at[d], seg_recv.at[d]).wait()
        for s in range(1, depth):
            push(s, g)
            if s == depth - 1 and g + 1 < groups:
                push(0, g + 1)

            @pl.when(wanted(s, 0))
            def _():
                attend(s, 0, g, False)
            attend_y(s - 1, g)
        if depth == 1 and g + 1 < groups:
            push(0, g + 1)
        attend_y(depth - 1, g)
        finish(g)

    for s in range(depth):
        for g in range(groups):
            for w in range(2):
                if s + 1 < depth:
                    @pl.when(sends_z(s))
                    def _():
                        z_copy(s, g, w).wait_send()
                for e in range(1, ny):
                    @pl.when(sends_y(s, e))
                    def _():
                        y_copy(s, e, g, w).wait_send()
    for d in range(1, reach + 1):
        @pl.when(me + d < n)
        def _():
            seg_copy(d).wait_send()
    for c in range(groups * pieces):
        o_own(c).wait()
        for e in range(1, tp):
            o_copy(c, e).wait()


def local(ny, queries, keys, values, segment_ids):
    rows, heads, head = queries.shape
    groups = keys.shape[1]
    per_group = heads // groups
    n = lax.axis_size("ctx")
    tp = lax.axis_size("tp")
    nz = n // ny
    longest = rows * n * 5 // 8
    reach = min((longest + rows - 1) // rows, n - 1)
    depth = min(nz - 1, (reach + ny - 1) // ny) + 1
    q = jnp.transpose(queries, (1, 0, 2))
    kv = jnp.transpose(jnp.stack([keys, values]), (2, 0, 1, 3))
    pieces = groups * (per_group // max(per_group // 2, 1))
    slots = depth * ny
    vmem = pl.BlockSpec(memory_space=pltpu.VMEM)
    dma = pltpu.SemaphoreType.DMA
    cfg = (n, ny, reach, tp, groups, per_group, rows, head)
    return pl.pallas_call(
        functools.partial(kernel, cfg),
        out_shape=jax.ShapeDtypeStruct((rows // tp, tp * heads * head), jnp.bfloat16),
        in_specs=[vmem] * 4,
        out_specs=vmem,
        scratch_shapes=[
            pltpu.VMEM((slots, groups, 2, rows, head), jnp.bfloat16),
            pltpu.VMEM((reach + 1, 1, rows), jnp.int32),
            pltpu.VMEM((rows, rows), jnp.float32),
            pltpu.VMEM((heads, rows, 2 * head), jnp.float32),
            pltpu.VMEM((heads, rows, head), jnp.float32),
            pltpu.VMEM((rows, heads * head), jnp.bfloat16),
            dma((slots * groups * 2,)),
            dma((slots * groups * 2,)),
            dma((reach + 1,)),
            dma((reach + 1,)),
            dma((pieces * tp,)),
            dma((pieces * tp,)),
            dma((pieces,)),
        ],
        compiler_params=pltpu.CompilerParams(
            collective_id=0, has_side_effects=True, vmem_limit_bytes=56 * 1024 * 1024
        ),
    )(q, kv, segment_ids.reshape(1, rows), segment_ids.reshape(rows, 1))


def solution(mesh):
    in_specs = (P("ctx", "tp", None), P("ctx", "tp", None), P("ctx", "tp", None), P("ctx"))
    out_specs = P(("ctx", "tp"), None)
    body = functools.partial(local, plane_width(mesh))
    return jax.shard_map(body, mesh=mesh, in_specs=in_specs, out_specs=out_specs, check_vma=False)
```

```python
import functools
import math

import jax
import jax.numpy as jnp
from jax import lax
from jax.experimental import pallas as pl
from jax.experimental.pallas import tpu as pltpu
from jax.sharding import PartitionSpec as P

MESH = pl.DeviceIdType.MESH
NEG = -1e30


def plane_width(mesh):
    n = mesh.shape["ctx"]
    try:
        width = len({d.coords[1] for d in mesh.devices.flat})
    except Exception:
        width = 2
    return width if n % width == 0 else 1


def kernel(cfg, q_ref, k_in, v_in, seg_ref, out_ref,
           buf, segs, segcol, bias, acc, top, o_buf,
           kv_send, kv_recv, seg_send, seg_recv, o_send, o_recv, o_local):
    n, ny, reach, tp, groups, per_group, rows, head = cfg
    nz = n // ny
    depth = min(nz - 1, (reach + ny - 1) // ny) + 1
    out_rows = rows // tp
    const = math.log2(math.e) / math.sqrt(head)
    me = lax.axis_index("ctx")
    mt = lax.axis_index("tp")
    z = me // ny
    y = me % ny

    barrier = pltpu.get_barrier_semaphore()
    for d in range(1, reach + 1):
        @pl.when(me + d < n)
        def _():
            pl.semaphore_signal(barrier, inc=1, device_id={"ctx": me + d, "tp": mt}, device_id_type=MESH)

        @pl.when(me - d >= 0)
        def _():
            pl.semaphore_signal(barrier, inc=1, device_id={"ctx": me - d, "tp": mt}, device_id_type=MESH)
    for e in range(1, tp):
        pl.semaphore_signal(barrier, inc=1, device_id={"ctx": me, "tp": (mt + e) % tp}, device_id_type=MESH)
    peers = (tp - 1) + jnp.minimum(n - 1 - me, reach) + jnp.minimum(me, reach)
    pl.semaphore_wait(barrier, peers)

    def piece(s, dy, g, w):
        if s == 0 and dy == 0:
            return (k_in, v_in)[w].at[g]
        return buf.at[s * ny + dy, g, w]

    def sem_index(s, dy, g, w):
        return ((s * ny + dy) * groups + g) * 2 + w

    def send_index(s, e, g, w):
        return ((s * ny + e) * groups + g) * 2 + w

    def z_copy(s, g, w):
        return pltpu.make_async_remote_copy(
            src_ref=piece(s, 0, g, w),
            dst_ref=buf.at[(s + 1) * ny, g, w],
            send_sem=kv_send.at[send_index(s, 0, g, w)],
            recv_sem=kv_recv.at[sem_index(s + 1, 0, g, w)],
            device_id={"ctx": me + ny, "tp": mt},
            device_id_type=MESH,
        )

    def y_copy(s, e, g, w):
        return pltpu.make_async_remote_copy(
            src_ref=piece(s, 0, g, w),
            dst_ref=buf.at[s * ny + ny - e, g, w],
            send_sem=kv_send.at[send_index(s, e, g, w)],
            recv_sem=kv_recv.at[sem_index(s, ny - e, g, w)],
            device_id={"ctx": z * ny + (y + e) % ny, "tp": mt},
            device_id_type=MESH,
        )

    def owner(s, dy):
        return (z - s) * ny + (y + dy) % ny

    def has_column(s):
        return (z >= s) & (z * ny - owner(s, 0) <= reach)

    def sends_z(s):
        return (z >= s) & (z + 1 < nz) & ((z + 1) * ny - owner(s, 0) <= reach)

    def sends_y(s, e):
        gap = z * ny + (y + e) % ny - owner(s, 0)
        return (z >= s) & (gap > 0) & (gap <= reach)

    def wanted(s, dy):
        gap = me - owner(s, dy)
        return (z >= s) & (gap > 0) & (gap <= reach)

    def arrived(s, dy, g, w):
        pltpu.make_async_copy(buf.at[s * ny + dy, g, w], buf.at[s * ny + dy, g, w],
                              kv_recv.at[sem_index(s, dy, g, w)]).wait()

    def push(s, g):
        for w in range(2):
            if s > 0:
                @pl.when(has_column(s))
                def _():
                    arrived(s, 0, g, w)
            if s + 1 < depth:
                @pl.when(sends_z(s))
                def _():
                    z_copy(s, g, w).start()
            for e in range(1, ny):
                @pl.when(sends_y(s, e))
                def _():
                    y_copy(s, e, g, w).start()

    def seg_copy(d):
        return pltpu.make_async_remote_copy(
            src_ref=seg_ref,
            dst_ref=segs.at[d],
            send_sem=seg_send.at[d],
            recv_sem=seg_recv.at[d],
            device_id={"ctx": me + d, "tp": mt},
            device_id_type=MESH,
        )

    push(0, 0)
    for d in range(1, reach + 1):
        @pl.when(me + d < n)
        def _():
            seg_copy(d).start()

    segcol[...] = jnp.transpose(jnp.broadcast_to(seg_ref[...], (head, rows)))

    def attend(s, dy, g, first):
        k_ref, v_ref = piece(s, dy, g, 0), piece(s, dy, g, 1)
        if first:
            seg_k = seg_ref[...]
        else:
            seg_k = segs[me - owner(s, dy)]
        column = segcol[...]
        allowed = jnp.concatenate([column] * (rows // head), axis=1) == seg_k
        if first:
            r = lax.broadcasted_iota(jnp.int32, (rows, rows), 0)
            c = lax.broadcasted_iota(jnp.int32, (rows, rows), 1)
            allowed = allowed & (c <= r)
        bias[...] = jnp.where(allowed, 0.0, NEG)

        def one(h, carry):
            i = g * per_group + h
            scores = lax.dot_general(q_ref[i], k_ref[...], (((1,), (1,)), ((), ())),
                                     preferred_element_type=jnp.float32)
            scores = scores * const + bias[...]
            high = jnp.broadcast_to(jnp.max(scores, axis=1, keepdims=True), (rows, head))
            if not first:
                old = top[i]
                high = jnp.maximum(old, high)
            weights = jnp.exp2(scores - jnp.concatenate([high] * (rows // head), axis=1)).astype(jnp.bfloat16)
            v = jnp.concatenate([v_ref[...], jnp.ones((rows, head), jnp.bfloat16)], axis=1)
            mixed = jnp.dot(weights, v, preferred_element_type=jnp.float32)
            if not first:
                factor = jnp.exp2(old - high)
                mixed = acc[i] * jnp.concatenate([factor, factor], axis=1) + mixed
            acc[i] = mixed
            top[i] = high
            return carry

        lax.fori_loop(0, per_group, one, 0, unroll=per_group)

    def attend_y(s, g):
        for dy in range(1, ny):
            @pl.when(wanted(s, dy))
            def _():
                arrived(s, dy, g, 0)
                arrived(s, dy, g, 1)
                attend(s, dy, g, False)

    per_send = max(per_group // 2, 1)
    width = per_send * head
    pieces = per_group // per_send

    def o_copy(c, e):
        col = pl.multiple_of((mt * groups * pieces + c) * width, width)
        to = (mt + e) % tp
        return pltpu.make_async_remote_copy(
            src_ref=o_buf.at[pl.ds(pl.multiple_of(to * out_rows, out_rows), out_rows), pl.ds(c * width, width)],
            dst_ref=out_ref.at[:, pl.ds(col, width)],
            send_sem=o_send.at[c * tp + e],
            recv_sem=o_recv.at[c * tp + e],
            device_id={"ctx": me, "tp": to},
            device_id_type=MESH,
        )

    def o_own(c):
        col = pl.multiple_of((mt * groups * pieces + c) * width, width)
        return pltpu.make_async_copy(
            o_buf.at[pl.ds(pl.multiple_of(mt * out_rows, out_rows), out_rows), pl.ds(c * width, width)],
            out_ref.at[:, pl.ds(col, width)],
            o_local.at[c],
        )

    def finish(g):
        for p in range(pieces):
            c = g * pieces + p
            for h in range(per_send):
                i = g * per_group + p * per_send + h
                o_buf[:, i * head:(i + 1) * head] = (acc[i, :, :head] / acc[i, :, head:]).astype(jnp.bfloat16)
            for e in range(1, tp):
                o_copy(c, e).start()
            o_own(c).start()

    for g in range(groups):
        attend(0, 0, g, True)
        if g == 0:
            for d in range(1, reach + 1):
                @pl.when(me - d >= 0)
                def _():
                    pltpu.make_async_copy(segs.at[d], segs.at[d], seg_recv.at[d]).wait()
        for s in range(1, depth):
            push(s, g)
            if s == depth - 1 and g + 1 < groups:
                push(0, g + 1)

            @pl.when(wanted(s, 0))
            def _():
                attend(s, 0, g, False)
            attend_y(s - 1, g)
        if depth == 1 and g + 1 < groups:
            push(0, g + 1)
        attend_y(depth - 1, g)
        finish(g)

    for s in range(depth):
        for g in range(groups):
            for w in range(2):
                if s + 1 < depth:
                    @pl.when(sends_z(s))
                    def _():
                        z_copy(s, g, w).wait_send()
                for e in range(1, ny):
                    @pl.when(sends_y(s, e))
                    def _():
                        y_copy(s, e, g, w).wait_send()
    for d in range(1, reach + 1):
        @pl.when(me + d < n)
        def _():
            seg_copy(d).wait_send()
    for c in range(groups * pieces):
        o_own(c).wait()
        for e in range(1, tp):
            o_copy(c, e).wait()


def local(ny, queries, keys, values, segment_ids):
    rows, heads, head = queries.shape
    groups = keys.shape[1]
    per_group = heads // groups
    n = lax.axis_size("ctx")
    tp = lax.axis_size("tp")
    nz = n // ny
    longest = rows * n * 5 // 8
    reach = min((longest + rows - 1) // rows, n - 1)
    depth = min(nz - 1, (reach + ny - 1) // ny) + 1
    q = jnp.transpose(queries, (1, 0, 2))
    k = jnp.transpose(keys, (1, 0, 2))
    v = jnp.transpose(values, (1, 0, 2))
    pieces = groups * (per_group // max(per_group // 2, 1))
    slots = depth * ny
    vmem = pl.BlockSpec(memory_space=pltpu.VMEM)
    dma = pltpu.SemaphoreType.DMA
    cfg = (n, ny, reach, tp, groups, per_group, rows, head)
    return pl.pallas_call(
        functools.partial(kernel, cfg),
        out_shape=jax.ShapeDtypeStruct((rows // tp, tp * heads * head), jnp.bfloat16),
        in_specs=[vmem] * 4,
        out_specs=vmem,
        scratch_shapes=[
            pltpu.VMEM((slots, groups, 2, rows, head), jnp.bfloat16),
            pltpu.VMEM((reach + 1, 1, rows), jnp.int32),
            pltpu.VMEM((rows, head), jnp.int32),
            pltpu.VMEM((rows, rows), jnp.float32),
            pltpu.VMEM((heads, rows, 2 * head), jnp.float32),
            pltpu.VMEM((heads, rows, head), jnp.float32),
            pltpu.VMEM((rows, heads * head), jnp.bfloat16),
            dma((slots * groups * 2,)),
            dma((slots * groups * 2,)),
            dma((reach + 1,)),
            dma((reach + 1,)),
            dma((pieces * tp,)),
            dma((pieces * tp,)),
            dma((pieces,)),
        ],
        compiler_params=pltpu.CompilerParams(
            collective_id=0, has_side_effects=True, vmem_limit_bytes=56 * 1024 * 1024
        ),
    )(q, k, v, segment_ids.reshape(1, rows))


def solution(mesh):
    in_specs = (P("ctx", "tp", None), P("ctx", "tp", None), P("ctx", "tp", None), P("ctx"))
    out_specs = P(("ctx", "tp"), None)
    body = functools.partial(local, plane_width(mesh))
    return jax.shard_map(body, mesh=mesh, in_specs=in_specs, out_specs=out_specs, check_vma=False)
```

```python
import functools
import math

import jax
import jax.numpy as jnp
from jax import lax
from jax.experimental import pallas as pl
from jax.experimental.pallas import tpu as pltpu
from jax.sharding import PartitionSpec as P

MESH = pl.DeviceIdType.MESH
NEG = -1e30


def plane_width(mesh):
    n = mesh.shape["ctx"]
    try:
        width = len({d.coords[1] for d in mesh.devices.flat})
    except Exception:
        width = 2
    return width if n % width == 0 else 1


def kernel(cfg, q_in, k_in, v_in, seg_ref, out_ref,
           q_ref, buf, segs, segcol, bias, acc, top, o_buf,
           kv_send, kv_recv, seg_send, seg_recv, o_send, o_recv, o_local):
    n, ny, reach, tp, groups, per_group, rows, head = cfg
    nz = n // ny
    depth = min(nz - 1, (reach + ny - 1) // ny) + 1
    out_rows = rows // tp
    const = math.log2(math.e) / math.sqrt(head)
    me = lax.axis_index("ctx")
    mt = lax.axis_index("tp")
    z = me // ny
    y = me % ny

    barrier = pltpu.get_barrier_semaphore()
    for d in range(1, reach + 1):
        @pl.when(me + d < n)
        def _():
            pl.semaphore_signal(barrier, inc=1, device_id={"ctx": me + d, "tp": mt}, device_id_type=MESH)

        @pl.when(me - d >= 0)
        def _():
            pl.semaphore_signal(barrier, inc=1, device_id={"ctx": me - d, "tp": mt}, device_id_type=MESH)
    for e in range(1, tp):
        pl.semaphore_signal(barrier, inc=1, device_id={"ctx": me, "tp": (mt + e) % tp}, device_id_type=MESH)
    peers = (tp - 1) + jnp.minimum(n - 1 - me, reach) + jnp.minimum(me, reach)
    pl.semaphore_wait(barrier, peers)

    def piece(s, dy, g, w):
        if s == 0 and dy == 0:
            return (k_in, v_in)[w].at[g]
        return buf.at[s * ny + dy, g, w]

    def sem_index(s, dy, g, w):
        return ((s * ny + dy) * groups + g) * 2 + w

    def send_index(s, e, g, w):
        return ((s * ny + e) * groups + g) * 2 + w

    def z_copy(s, g, w):
        return pltpu.make_async_remote_copy(
            src_ref=piece(s, 0, g, w),
            dst_ref=buf.at[(s + 1) * ny, g, w],
            send_sem=kv_send.at[send_index(s, 0, g, w)],
            recv_sem=kv_recv.at[sem_index(s + 1, 0, g, w)],
            device_id={"ctx": me + ny, "tp": mt},
            device_id_type=MESH,
        )

    def y_copy(s, e, g, w):
        return pltpu.make_async_remote_copy(
            src_ref=piece(s, 0, g, w),
            dst_ref=buf.at[s * ny + ny - e, g, w],
            send_sem=kv_send.at[send_index(s, e, g, w)],
            recv_sem=kv_recv.at[sem_index(s, ny - e, g, w)],
            device_id={"ctx": z * ny + (y + e) % ny, "tp": mt},
            device_id_type=MESH,
        )

    last = depth - 1
    straight = last >= 2 and last * ny > reach

    def far_copy(dy, g, w):
        return pltpu.make_async_remote_copy(
            src_ref=piece(last - 1, dy, g, w),
            dst_ref=buf.at[last * ny + dy, g, w],
            send_sem=kv_send.at[send_index(last, dy, g, w)],
            recv_sem=kv_recv.at[sem_index(last, dy, g, w)],
            device_id={"ctx": me + ny, "tp": mt},
            device_id_type=MESH,
        )

    def sends_far(dy):
        gap = me + ny - owner(last - 1, dy)
        return (z >= last - 1) & (z + 1 < nz) & (gap <= reach)

    def owner(s, dy):
        return (z - s) * ny + (y + dy) % ny

    def has_column(s):
        return (z >= s) & (s * ny <= reach)

    def sends_z(s):
        return (z >= s) & (z + 1 < nz) & ((s + 1) * ny <= reach)

    def sends_y(s, e):
        gap = z * ny + (y + e) % ny - owner(s, 0)
        return (z >= s) & (s * ny <= reach) & (gap > 0) & (gap <= reach)

    def wanted(s, dy):
        gap = me - owner(s, dy)
        return (z >= s) & (gap > 0) & (gap <= reach)

    def arrived(s, dy, g, w):
        pltpu.make_async_copy(buf.at[s * ny + dy, g, w], buf.at[s * ny + dy, g, w],
                              kv_recv.at[sem_index(s, dy, g, w)]).wait()

    def push(s, g):
        for w in range(2):
            if s > 0:
                @pl.when(has_column(s))
                def _():
                    arrived(s, 0, g, w)
            if s + 1 < depth:
                @pl.when(sends_z(s))
                def _():
                    z_copy(s, g, w).start()
            for e in range(1, ny):
                @pl.when(sends_y(s, e))
                def _():
                    y_copy(s, e, g, w).start()

    def seg_copy(d):
        return pltpu.make_async_remote_copy(
            src_ref=seg_ref,
            dst_ref=segs.at[d],
            send_sem=seg_send.at[d],
            recv_sem=seg_recv.at[d],
            device_id={"ctx": me + d, "tp": mt},
            device_id_type=MESH,
        )

    push(0, 0)
    for d in range(1, reach + 1):
        @pl.when(me + d < n)
        def _():
            seg_copy(d).start()

    for i in range(groups * per_group):
        q_ref[i] = q_in[:, i, :]
    segcol[...] = jnp.transpose(jnp.broadcast_to(seg_ref[...], (head, rows)))

    def attend(s, dy, g, first):
        k_ref, v_ref = piece(s, dy, g, 0), piece(s, dy, g, 1)
        if first:
            seg_k = seg_ref[...]
        else:
            seg_k = segs[me - owner(s, dy)]
        column = segcol[...]
        allowed = jnp.concatenate([column] * (rows // head), axis=1) == seg_k
        if first:
            r = lax.broadcasted_iota(jnp.int32, (rows, rows), 0)
            c = lax.broadcasted_iota(jnp.int32, (rows, rows), 1)
            allowed = allowed & (c <= r)
        bias[...] = jnp.where(allowed, 0.0, NEG)

        def one(h, carry):
            i = g * per_group + h
            scores = lax.dot_general(q_ref[i], k_ref[...], (((1,), (1,)), ((), ())),
                                     preferred_element_type=jnp.float32)
            scores = scores * const + bias[...]
            high = jnp.broadcast_to(jnp.max(scores, axis=1, keepdims=True), (rows, head))
            if not first:
                old = top[i]
                high = jnp.maximum(old, high)
            weights = jnp.exp2(scores - jnp.concatenate([high] * (rows // head), axis=1)).astype(jnp.bfloat16)
            v = jnp.concatenate([v_ref[...], jnp.ones((rows, head), jnp.bfloat16)], axis=1)
            mixed = jnp.dot(weights, v, preferred_element_type=jnp.float32)
            if not first:
                factor = jnp.exp2(old - high)
                mixed = acc[i] * jnp.concatenate([factor, factor], axis=1) + mixed
            acc[i] = mixed
            top[i] = high
            return carry

        lax.fori_loop(0, per_group, one, 0, unroll=per_group)

    def attend_y(s, g):
        for dy in range(1, ny):
            @pl.when(wanted(s, dy))
            def _():
                arrived(s, dy, g, 0)
                arrived(s, dy, g, 1)
                if straight and s == last - 1:
                    @pl.when(sends_far(dy))
                    def _():
                        far_copy(dy, g, 0).start()
                        far_copy(dy, g, 1).start()
                attend(s, dy, g, False)

    per_send = max(per_group // 2, 1)
    width = per_send * head
    pieces = per_group // per_send

    def o_copy(c, e):
        col = pl.multiple_of((mt * groups * pieces + c) * width, width)
        to = (mt + e) % tp
        return pltpu.make_async_remote_copy(
            src_ref=o_buf.at[pl.ds(pl.multiple_of(to * out_rows, out_rows), out_rows), pl.ds(c * width, width)],
            dst_ref=out_ref.at[:, pl.ds(col, width)],
            send_sem=o_send.at[c * tp + e],
            recv_sem=o_recv.at[c * tp + e],
            device_id={"ctx": me, "tp": to},
            device_id_type=MESH,
        )

    def o_own(c):
        col = pl.multiple_of((mt * groups * pieces + c) * width, width)
        return pltpu.make_async_copy(
            o_buf.at[pl.ds(pl.multiple_of(mt * out_rows, out_rows), out_rows), pl.ds(c * width, width)],
            out_ref.at[:, pl.ds(col, width)],
            o_local.at[c],
        )

    def finish(g):
        for p in range(pieces):
            c = g * pieces + p
            for h in range(per_send):
                i = g * per_group + p * per_send + h
                o_buf[:, i * head:(i + 1) * head] = (acc[i, :, :head] / acc[i, :, head:]).astype(jnp.bfloat16)
            for e in range(1, tp):
                o_copy(c, e).start()
            o_own(c).start()

    for g in range(groups):
        attend(0, 0, g, True)
        if g == 0:
            for d in range(1, reach + 1):
                @pl.when(me - d >= 0)
                def _():
                    pltpu.make_async_copy(segs.at[d], segs.at[d], seg_recv.at[d]).wait()
        for s in range(1, depth):
            push(s, g)
            if s == depth - 1 and g + 1 < groups:
                push(0, g + 1)

            @pl.when(wanted(s, 0))
            def _():
                attend(s, 0, g, False)
            attend_y(s - 1, g)
        if depth == 1 and g + 1 < groups:
            push(0, g + 1)
        attend_y(depth - 1, g)
        finish(g)

    for s in range(depth):
        for g in range(groups):
            for w in range(2):
                if s + 1 < depth:
                    @pl.when(sends_z(s))
                    def _():
                        z_copy(s, g, w).wait_send()
                for e in range(1, ny):
                    @pl.when(sends_y(s, e))
                    def _():
                        y_copy(s, e, g, w).wait_send()
    if straight:
        for g in range(groups):
            for w in range(2):
                for dy in range(1, ny):
                    @pl.when(wanted(last - 1, dy) & sends_far(dy))
                    def _():
                        far_copy(dy, g, w).wait_send()
    for d in range(1, reach + 1):
        @pl.when(me + d < n)
        def _():
            seg_copy(d).wait_send()
    for c in range(groups * pieces):
        o_own(c).wait()
        for e in range(1, tp):
            o_copy(c, e).wait()


def local(ny, queries, keys, values, segment_ids):
    rows, heads, head = queries.shape
    groups = keys.shape[1]
    per_group = heads // groups
    n = lax.axis_size("ctx")
    tp = lax.axis_size("tp")
    nz = n // ny
    longest = rows * n * 5 // 8
    reach = min((longest + rows - 1) // rows, n - 1)
    depth = min(nz - 1, (reach + ny - 1) // ny) + 1
    k = jnp.transpose(keys, (1, 0, 2))
    v = jnp.transpose(values, (1, 0, 2))
    pieces = groups * (per_group // max(per_group // 2, 1))
    slots = depth * ny
    vmem = pl.BlockSpec(memory_space=pltpu.VMEM)
    dma = pltpu.SemaphoreType.DMA
    cfg = (n, ny, reach, tp, groups, per_group, rows, head)
    return pl.pallas_call(
        functools.partial(kernel, cfg),
        out_shape=jax.ShapeDtypeStruct((rows // tp, tp * heads * head), jnp.bfloat16),
        in_specs=[vmem] * 4,
        out_specs=vmem,
        scratch_shapes=[
            pltpu.VMEM((heads, rows, head), jnp.bfloat16),
            pltpu.VMEM((slots, groups, 2, rows, head), jnp.bfloat16),
            pltpu.VMEM((reach + 1, 1, rows), jnp.int32),
            pltpu.VMEM((rows, head), jnp.int32),
            pltpu.VMEM((rows, rows), jnp.float32),
            pltpu.VMEM((heads, rows, 2 * head), jnp.float32),
            pltpu.VMEM((heads, rows, head), jnp.float32),
            pltpu.VMEM((rows, heads * head), jnp.bfloat16),
            dma((slots * groups * 2,)),
            dma((slots * groups * 2,)),
            dma((reach + 1,)),
            dma((reach + 1,)),
            dma((pieces * tp,)),
            dma((pieces * tp,)),
            dma((pieces,)),
        ],
        compiler_params=pltpu.CompilerParams(
            collective_id=0, has_side_effects=True, vmem_limit_bytes=56 * 1024 * 1024
        ),
    )(queries, k, v, segment_ids.reshape(1, rows))


def solution(mesh):
    in_specs = (P("ctx", "tp", None), P("ctx", "tp", None), P("ctx", "tp", None), P("ctx"))
    out_specs = P(("ctx", "tp"), None)
    body = functools.partial(local, plane_width(mesh))
    return jax.shard_map(body, mesh=mesh, in_specs=in_specs, out_specs=out_specs, check_vma=False)
```
